256 devices in a mesh: site: 4 (over y), rows: 4 (over z_lo), cols: 4 (over z_hi, core), slabs: 4 (over x).
Axes of the slice: x: 4, y: 4, z: 8 (z_hi: 2, z_lo: 4; z = z_hi * 4 + z_lo), core: 2. Of those that a mesh axis runs over, the one named last changes fastest.
Arguments:
- pressure: float32 [64, 256, 128, 128], P(('site', 'rows'), 'cols', 'slabs'), parts along dimension 0, may hold values from 0.2 to 1.8
- earlier: float32 [64, 256, 128, 128], P(('site', 'rows'), 'cols', 'slabs'), parts along dimension 0, may hold values from 0.2 to 1.8
- speed_square: float32 [64, 256, 128, 128], P(('site', 'rows'), 'cols', 'slabs'), parts along dimension 0, may hold values from 0.05 to 0.3
Outputs:
- potential: float32 [64, 256, 128, 128], P(('site', 'rows'), 'cols', 'slabs'), parts along dimension 0
- pressure_end: float32 [64, 256, 128, 128], P(('site', 'rows'), 'cols', 'slabs'), parts along dimension 0
The draws below stay inside these ranges and needn't reach their ends.
There are 4 independent parts, one for each index of `site`. The reference program is written for one: setup_inputs(seed, part) draws one part's arguments, and reference() takes and returns one part's arrays. A program takes and returns all parts, laid end to end along the dimension named above; each array names one. Nothing has to cross between parts.
All inputs are finite; a program needn't handle non-finite values.
Results may differ from the reference program's by a relative error of at most 0.00002.
Values sent between devices are 32-bit elements; how exact they have to be, the bound alone decides.
No kernel may reach another device: no remote copies, remote signals or barrier semaphores. Data moves between devices by JAX's collectives and lax.ppermute only.
A program may use at most 192 MiB of HBM per device.

```python
import jax
import jax.numpy as jnp
from jax import lax

GRID_J = 16
GRID_I = 256
GRID_K = 128
MEMBERS = 128
STEPS = 4


def steps_of(rng, extent, split, low, high):
    def one(dim, shards_of):
        draws = jax.random.uniform(jax.random.fold_in(jax.random.fold_in(rng, 6), dim), (shards_of,), jnp.float32, low / len(split), high / len(split))
        return jnp.repeat(jnp.exp(draws), extent[dim] // shards_of).reshape((-1,) + (1,) * (len(extent) - dim - 1))

    gain = one(*split[0])
    for cut in split[1:]:
        gain = gain * one(*cut)
    return gain


def setup_inputs(seed: int = 0, part: int = 0) -> dict:
    key_list = jax.random.split(jax.random.key(seed), 4)
    part_keys = jax.random.split(jax.random.fold_in(key_list[3], part), 4)
    return {
        "pressure": jnp.clip(0.2 + 1.5999999 * jax.random.uniform(part_keys[0], (GRID_J, GRID_I, GRID_K, MEMBERS), jnp.float32) ** steps_of(part_keys[0], (GRID_J, GRID_I, GRID_K, MEMBERS), ((0, 4), (1, 4), (2, 4)), -0.2, 0.2), 0.2, 1.8),
        "earlier": jnp.clip(0.2 + 1.5999999 * jax.random.uniform(part_keys[1], (GRID_J, GRID_I, GRID_K, MEMBERS), jnp.float32) ** steps_of(part_keys[1], (GRID_J, GRID_I, GRID_K, MEMBERS), ((0, 4), (1, 4), (2, 4)), -0.2, 0.2), 0.2, 1.8),
        "speed_square": jnp.clip(0.05 + 0.25 * jax.random.uniform(part_keys[2], (GRID_J, GRID_I, GRID_K, MEMBERS), jnp.float32) ** steps_of(part_keys[2], (GRID_J, GRID_I, GRID_K, MEMBERS), ((0, 4), (1, 4), (2, 4)), -0.2, 0.2), 0.05, 0.3),
    }


def strip_edges(values, dims):
    for dim in dims:
        values = lax.slice_in_dim(values, 1, values.shape[dim] - 1, axis=dim)
    return values


def neighbour(values, dim, start, dims):
    others = [other for other in dims if other != dim]
    values = strip_edges(values, others)
    return lax.slice_in_dim(values, start, start + values.shape[dim] - 2, axis=dim)


def one_step(padded, before, speed_square):
    middle = strip_edges(padded, (0, 1, 2))
    lower = [neighbour(padded, dim, 0, (0, 1, 2)) for dim in (0, 1, 2)]
    upper = [neighbour(padded, dim, 2, (0, 1, 2)) for dim in (0, 1, 2)]
    spread = lower[0] + upper[0] + lower[1] + upper[1] + lower[2] + upper[2] - 6.0 * middle
    return 2.0 * middle - before + speed_square * spread


def reference(pressure, earlier, speed_square):
    for step in range(STEPS):
        later = one_step(jnp.pad(pressure, ((1, 1), (1, 1), (1, 1), (0, 0)), mode="wrap"), earlier, speed_square)
        earlier, pressure = pressure, later
    potential = jnp.cumsum(pressure, axis=0) / GRID_J
    return potential, pressure
```

```python
import functools

import jax
import jax.numpy as jnp
from jax import lax
from jax.experimental import pallas as pl
from jax.experimental.pallas import tpu as pltpu
from jax.sharding import PartitionSpec as P


STEPS = 4
GRID_J = 16
WIDTHS = (32, 24, 8)
GROUP = 8


def step_kernel(refs, *, start, width, first, last, final, has_dst):
    n = iter(range(len(refs)))

    def take():
        return refs[next(n)]

    p_hbm, e_hbm, c_hbm, lo_hbm, hi_hbm, klo_hbm, khi_hbm = (take() for _ in range(7))
    ilo = take() if first else p_hbm.at[:, pl.ds(start - 1, 1)]
    ihi = take() if last else p_hbm.at[:, pl.ds(start + width, 1)]
    if has_dst:
        take()
    out_hbm = take()
    if final:
        tot_hbm = take()
    else:
        dn_hbm, up_hbm, kfirst_hbm, klast_hbm = (take() for _ in range(4))
        ifirst_hbm = take() if first else None
        ilast_hbm = take() if last else None
    pbuf, ebuf, cbuf, rbuf, kbuf, psem, esem, csem, osem, rsem, ksem = (take() for _ in range(11))
    rows, depth = pbuf.shape[0], pbuf.shape[2]
    groups = width // GROUP

    def field(g, which):
        there = pl.ds(start + GROUP * g, GROUP)
        src, buf, shift, sem = (
            (p_hbm, pbuf, 1, psem),
            (e_hbm, ebuf, 0, esem),
            (c_hbm, cbuf, 0, csem),
        )[which]
        return pltpu.make_async_copy(
            src.at[:, there], buf.at[:, pl.ds(GROUP * g + shift, GROUP)], sem.at[g]
        )

    def result(g):
        mine = pl.ds(GROUP * g, GROUP)
        return pltpu.make_async_copy(
            ebuf.at[:, mine], out_hbm.at[:, pl.ds(start + GROUP * g, GROUP)], osem.at[g]
        )

    ends = [
        pltpu.make_async_copy(ilo, pbuf.at[:, pl.ds(0, 1)], ksem.at[2]),
        pltpu.make_async_copy(ihi, pbuf.at[:, pl.ds(width + 1, 1)], ksem.at[3]),
        pltpu.make_async_copy(klo_hbm, kbuf.at[0], ksem.at[0]),
        pltpu.make_async_copy(khi_hbm, kbuf.at[1], ksem.at[1]),
        pltpu.make_async_copy(lo_hbm, rbuf.at[0], rsem.at[0]),
        pltpu.make_async_copy(hi_hbm, rbuf.at[1], rsem.at[1]),
    ]
    for which in range(3):
        field(0, which).start()
    for cp in ends:
        cp.start()
    for g in range(1, groups):
        for which in range(3):
            field(g, which).start()
    k = lax.broadcasted_iota(jnp.int32, (depth, pbuf.shape[3]), 0)
    is_first, is_last = k == 0, k == depth - 1
    for cp in ends:
        cp.wait()
    field(0, 0).wait()

    def group(g, _):
        @pl.when(g + 1 < groups)
        def _():
            field(g + 1, 0).wait()

        field(g, 1).wait()
        field(g, 2).wait()

        def column(n, _):
            i = GROUP * g + n
            mid = [pbuf[j, i + 1] for j in range(rows)]
            acc = None
            for j in range(rows):
                x = mid[j]
                low = rbuf[0, i] if j == 0 else mid[j - 1]
                high = rbuf[1, i] if j == rows - 1 else mid[j + 1]
                below = jnp.where(is_first, kbuf[0, j, pl.ds(i, 1), :], pltpu.roll(x, 1, 0))
                above = jnp.where(
                    is_last, kbuf[1, j, pl.ds(i, 1), :], pltpu.roll(x, depth - 1, 0)
                )
                spread = (
                    low + high + pbuf[j, i] + pbuf[j, i + 2] + below + above - 6.0 * x
                )
                new = 2.0 * x - ebuf[j, i] + cbuf[j, i] * spread
                ebuf[j, i] = new
                if final:
                    acc = new if acc is None else acc + new
                else:
                    kbuf[2, j, pl.ds(i, 1), :] = new[0:1]
                    kbuf[3, j, pl.ds(i, 1), :] = new[depth - 1 : depth]
            if final:
                rbuf[2, i] = acc
            return 0

        lax.fori_loop(0, GROUP, column, 0)
        result(g).start()
        return 0

    lax.fori_loop(0, groups, group, 0)
    if final:
        edges = [pltpu.make_async_copy(rbuf.at[2], tot_hbm, rsem.at[2])]
    else:
        edges = [
            pltpu.make_async_copy(ebuf.at[0], dn_hbm, rsem.at[2]),
            pltpu.make_async_copy(ebuf.at[rows - 1], up_hbm, rsem.at[3]),
            pltpu.make_async_copy(kbuf.at[2], kfirst_hbm, ksem.at[4]),
            pltpu.make_async_copy(kbuf.at[3], klast_hbm, ksem.at[5]),
        ]
        if first:
            edges.append(pltpu.make_async_copy(ebuf.at[:, pl.ds(0, 1)], ifirst_hbm, ksem.at[6]))
        if last:
            edges.append(
                pltpu.make_async_copy(ebuf.at[:, pl.ds(width - 1, 1)], ilast_hbm, ksem.at[7])
            )
    for cp in edges:
        cp.start()
    for g in range(groups):
        result(g).wait()
    for cp in edges:
        cp.wait()


def step(p, e, c, halo, dst, *, start, width, final):
    rows, total, depth, lanes = p.shape
    first, last = start == 0, start + width == total
    args = [p, e, c, *halo]
    aliases = {}
    has_dst = dst is not None and dst is not e
    if dst is not None and not has_dst:
        aliases = {1: 0}
    elif has_dst:
        aliases = {len(args): 0}
        args.append(dst)
    f = jnp.float32
    outs = [jax.ShapeDtypeStruct(p.shape, f)]
    row = jax.ShapeDtypeStruct((width, depth, lanes), f)
    slab = jax.ShapeDtypeStruct((rows, width, lanes), f)
    col = jax.ShapeDtypeStruct((rows, 1, depth, lanes), f)
    if final:
        outs += [row]
    else:
        outs += [row, row, slab, slab] + [col] * first + [col] * last
    groups = width // GROUP
    cells = rows * width * depth * lanes

    def body(*refs):
        step_kernel(
            refs,
            start=start,
            width=width,
            first=first,
            last=last,
            final=final,
            has_dst=has_dst,
        )

    hbm = pl.BlockSpec(memory_space=pltpu.HBM)
    return pl.pallas_call(
        body,
        out_shape=outs,
        in_specs=[hbm] * len(args),
        out_specs=[hbm] * len(outs),
        scratch_shapes=[
            pltpu.VMEM((rows, width + 2, depth, lanes), f),
            pltpu.VMEM((rows, width, depth, lanes), f),
            pltpu.VMEM((rows, width, depth, lanes), f),
            pltpu.VMEM((3 if final else 2, width, depth, lanes), f),
            pltpu.VMEM((4, rows, width, lanes), f),
        ]
        + [pltpu.SemaphoreType.DMA((groups,))] * 4
        + [pltpu.SemaphoreType.DMA((4,)), pltpu.SemaphoreType.DMA((8,))],
        input_output_aliases=aliases,
        cost_estimate=pl.CostEstimate(
            flops=cells * 40, bytes_accessed=cells * 16, transcendentals=0
        ),
        name="wave_step",
    )(*args)


def sums_kernel(p_hbm, *refs, start, width, count, has_dst):
    before_hbm = refs[:count]
    refs = refs[count + (1 if has_dst else 0) :]
    out_hbm, pbuf, bbuf, psem, osem, bsem = refs
    rows = pbuf.shape[0]
    groups = width // GROUP

    def field(g):
        return pltpu.make_async_copy(
            p_hbm.at[:, pl.ds(start + GROUP * g, GROUP)],
            pbuf.at[:, pl.ds(GROUP * g, GROUP)],
            psem.at[g],
        )

    def result(g):
        return pltpu.make_async_copy(
            pbuf.at[:, pl.ds(GROUP * g, GROUP)],
            out_hbm.at[:, pl.ds(start + GROUP * g, GROUP)],
            osem.at[g],
        )

    carried = [
        pltpu.make_async_copy(before_hbm[s], bbuf.at[s], bsem.at[s]) for s in range(count)
    ]
    for cp in carried:
        cp.start()
    for g in range(groups):
        field(g).start()
    for cp in carried:
        cp.wait()

    def group(g, _):
        field(g).wait()

        def column(n, _):
            i = GROUP * g + n
            acc = bbuf[0, i]
            for s in range(1, count):
                acc = acc + bbuf[s, i]
            for j in range(rows):
                acc = acc + pbuf[j, i]
                pbuf[j, i] = acc * (1.0 / GRID_J)
            return 0

        lax.fori_loop(0, GROUP, column, 0)
        result(g).start()
        return 0

    lax.fori_loop(0, groups, group, 0)
    for g in range(groups):
        result(g).wait()


def sums(p, before, dst, *, start, width):
    rows, _, depth, lanes = p.shape
    args = [p, *before]
    aliases = {}
    if dst is not None:
        aliases = {len(args): 0}
        args.append(dst)
    groups = width // GROUP
    cells = rows * width * depth * lanes
    hbm = pl.BlockSpec(memory_space=pltpu.HBM)
    return pl.pallas_call(
        functools.partial(
            sums_kernel,
            start=start,
            width=width,
            count=len(before),
            has_dst=dst is not None,
        ),
        out_shape=jax.ShapeDtypeStruct(p.shape, jnp.float32),
        in_specs=[hbm] * len(args),
        out_specs=hbm,
        scratch_shapes=[
            pltpu.VMEM((rows, width, depth, lanes), jnp.float32),
            pltpu.VMEM((len(before), width, depth, lanes), jnp.float32),
        ]
        + [pltpu.SemaphoreType.DMA((groups,))] * 2
        + [pltpu.SemaphoreType.DMA((len(before),))],
        input_output_aliases=aliases,
        cost_estimate=pl.CostEstimate(
            flops=cells * 10, bytes_accessed=cells * 8, transcendentals=0
        ),
        name="running_sums",
    )(*args)


def ring(axis, by):
    size = lax.axis_size(axis)
    return [(a, (a + by) % size) for a in range(size)]


def local(pressure, earlier, speed_square):
    rows, total, depth, _ = pressure.shape
    starts = [sum(WIDTHS[:a]) for a in range(len(WIDTHS))]
    chunks = list(zip(starts, WIDTHS))
    count = len(chunks)

    def send(value, axis, pairs):
        return lax.ppermute(value, axis, pairs)

    def exchange(edges, a):
        dn, up, kfirst, klast = edges[:4]
        got = [
            send(up, "rows", ring("rows", 1)),
            send(dn, "rows", ring("rows", -1)),
            send(klast, "slabs", ring("slabs", 1)),
            send(kfirst, "slabs", ring("slabs", -1)),
        ]
        rest = list(edges[4:])
        ihi = send(rest.pop(0), "cols", ring("cols", -1)) if a == 0 else None
        ilo = send(rest.pop(0), "cols", ring("cols", 1)) if a == count - 1 else None
        return got, ilo, ihi

    def start_edges(a):
        start, width = chunks[a]
        part = lax.slice_in_dim(pressure, start, start + width, axis=1)
        edges = [part[0], part[rows - 1], part[:, :, 0], part[:, :, depth - 1]]
        if a == 0:
            edges.append(pressure[:, :1])
        if a == count - 1:
            edges.append(pressure[:, total - 1 :])
        return edges

    halos = [exchange(start_edges(a), a) for a in range(count)]
    older, newer = earlier, pressure
    for t in range(STEPS):
        final = t == STEPS - 1
        fresh = None if t < 2 else older
        made = []
        for a, (start, width) in enumerate(chunks):
            halo = list(halos[a][0])
            if a == 0:
                halo.append(halos[count - 1][1])
            if a == count - 1:
                halo.append(halos[0][2])
            before = older if t < 2 else fresh
            fresh, *edges = step(
                newer,
                before,
                speed_square,
                halo,
                fresh,
                start=start,
                width=width,
                final=final,
            )
            made.append(edges if final else exchange(edges, a))
        older, newer = newer, fresh
        halos = made

    potential = None
    size = lax.axis_size("rows")
    for a, (start, width) in enumerate(chunks):
        own = halos[a][0]
        before = []
        if a < count - 1:
            carried = own
            for s in range(size - 1):
                got = send(carried, "rows", [(s, s + 1)])
                before.append(got)
                carried = own + got
        else:
            for by in range(1, size):
                pairs = [(s, s + by) for s in range(size - by)]
                before.append(send(own, "rows", pairs))
        potential = sums(newer, before, potential, start=start, width=width)
    return potential, newer


def solution(mesh):
    placed = P(("site", "rows"), "cols", "slabs", None)

    return jax.shard_map(
        local,
        mesh=mesh,
        in_specs=(placed, placed, placed),
        out_specs=(placed, placed),
        check_vma=False,
    )
```

```python
import functools

import jax
import jax.numpy as jnp
from jax import lax
from jax.experimental import pallas as pl
from jax.experimental.pallas import tpu as pltpu
from jax.sharding import PartitionSpec as P


STEPS = 4
GRID_J = 16
WIDTHS = (32, 24, 8)
WRAP = 16
GROUP = 8
PIECES = ((16, 16), (16, 8), (8,))


def step_kernel(refs, *, start, width, total, final, has_dst):
    n = iter(range(len(refs)))

    def take():
        return refs[next(n)]

    around = start + width > total
    own = total - start if around else width
    p_hbm, e_hbm, c_hbm, lo_hbm, hi_hbm, klo_hbm, khi_hbm = (take() for _ in range(7))
    ilo_hbm, ihi_hbm = (take(), take()) if around else (None, None)
    if has_dst:
        take()
    out_hbm = take()
    if final:
        tot_hbm = [take() for _ in final]
    else:
        dn_hbm, up_hbm, kfirst_hbm, klast_hbm = (take() for _ in range(4))
        ifirst_hbm, ilast_hbm = (take(), take()) if around else (None, None)
    pbuf, ebuf, cbuf, rbuf, kbuf, psem, esem, csem, osem, rsem, ksem = (take() for _ in range(11))
    rows, depth = pbuf.shape[0], pbuf.shape[2]
    groups = width // GROUP

    def column_of(g):
        return lax.rem(start + GROUP * g, total)

    def shift_of(g):
        if not around:
            return 1
        if isinstance(g, int):
            return 1 if GROUP * g < own else 3
        return jnp.where(GROUP * g < own, 1, 3)

    def field(g, which):
        there = pl.ds(column_of(g), GROUP)
        src, buf, shift, sem = (
            (p_hbm, pbuf, shift_of(g), psem),
            (e_hbm, ebuf, 0, esem),
            (c_hbm, cbuf, 0, csem),
        )[which]
        return pltpu.make_async_copy(
            src.at[:, there], buf.at[:, pl.ds(GROUP * g + shift, GROUP)], sem.at[g]
        )

    def result(g):
        mine = pl.ds(GROUP * g, GROUP)
        return pltpu.make_async_copy(
            ebuf.at[:, mine], out_hbm.at[:, pl.ds(column_of(g), GROUP)], osem.at[g]
        )

    edge = pbuf.shape[1] - 1
    ends = [
        pltpu.make_async_copy(
            p_hbm.at[:, pl.ds(start - 1, 1)], pbuf.at[:, pl.ds(0, 1)], ksem.at[2]
        ),
        pltpu.make_async_copy(
            p_hbm.at[:, pl.ds((start + width) % total, 1)],
            pbuf.at[:, pl.ds(edge, 1)],
            ksem.at[3],
        ),
        pltpu.make_async_copy(klo_hbm, kbuf.at[0], ksem.at[0]),
        pltpu.make_async_copy(khi_hbm, kbuf.at[1], ksem.at[1]),
        pltpu.make_async_copy(lo_hbm, rbuf.at[0], rsem.at[0]),
        pltpu.make_async_copy(hi_hbm, rbuf.at[1], rsem.at[1]),
    ]
    if around:
        ends += [
            pltpu.make_async_copy(ihi_hbm, pbuf.at[:, pl.ds(own + 1, 1)], ksem.at[8]),
            pltpu.make_async_copy(ilo_hbm, pbuf.at[:, pl.ds(own + 2, 1)], ksem.at[9]),
        ]
    for which in range(3):
        field(0, which).start()
    for cp in ends:
        cp.start()
    for g in range(1, groups):
        for which in range(3):
            field(g, which).start()
    k = lax.broadcasted_iota(jnp.int32, (depth, pbuf.shape[3]), 0)
    is_first, is_last = k == 0, k == depth - 1
    for cp in ends:
        cp.wait()
    field(0, 0).wait()

    def group(g, _):
        @pl.when(g + 1 < groups)
        def _():
            field(g + 1, 0).wait()

        field(g, 1).wait()
        field(g, 2).wait()

        def column(n, _):
            i = GROUP * g + n
            at = i + shift_of(g)
            mid = [pbuf[j, at] for j in range(rows)]
            acc = None
            for j in range(rows):
                x = mid[j]
                low = rbuf[0, i] if j == 0 else mid[j - 1]
                high = rbuf[1, i] if j == rows - 1 else mid[j + 1]
                below = jnp.where(is_first, kbuf[0, j, pl.ds(i, 1), :], pltpu.roll(x, 1, 0))
                above = jnp.where(
                    is_last, kbuf[1, j, pl.ds(i, 1), :], pltpu.roll(x, depth - 1, 0)
                )
                spread = (
                    low + high + pbuf[j, at - 1] + pbuf[j, at + 1] + below + above - 6.0 * x
                )
                new = 2.0 * x - ebuf[j, i] + cbuf[j, i] * spread
                ebuf[j, i] = new
                if final:
                    acc = new if acc is None else acc + new
                else:
                    kbuf[2, j, pl.ds(i, 1), :] = new[0:1]
                    kbuf[3, j, pl.ds(i, 1), :] = new[depth - 1 : depth]
            if final:
                rbuf[2, i] = acc
            return 0

        lax.fori_loop(0, GROUP, column, 0)
        result(g).start()
        return 0

    lax.fori_loop(0, groups, group, 0)
    if final:
        edges = [
            pltpu.make_async_copy(
                rbuf.at[2, pl.ds(sum(final[:a]), final[a])], tot_hbm[a], rsem.at[2 + a]
            )
            for a in range(len(final))
        ]
    else:
        edges = [
            pltpu.make_async_copy(ebuf.at[0], dn_hbm, rsem.at[2]),
            pltpu.make_async_copy(ebuf.at[rows - 1], up_hbm, rsem.at[3]),
            pltpu.make_async_copy(kbuf.at[2], kfirst_hbm, ksem.at[4]),
            pltpu.make_async_copy(kbuf.at[3], klast_hbm, ksem.at[5]),
        ]
        if around:
            edges += [
                pltpu.make_async_copy(ebuf.at[:, pl.ds(own, 1)], ifirst_hbm, ksem.at[6]),
                pltpu.make_async_copy(ebuf.at[:, pl.ds(own - 1, 1)], ilast_hbm, ksem.at[7]),
            ]
    for cp in edges:
        cp.start()
    for g in range(groups):
        result(g).wait()
    for cp in edges:
        cp.wait()


def step(p, e, c, halo, dst, *, start, width, final):
    rows, total, depth, lanes = p.shape
    around = start + width > total
    args = [p, e, c, *halo]
    aliases = {}
    has_dst = dst is not None and dst is not e
    if dst is not None and not has_dst:
        aliases = {1: 0}
    elif has_dst:
        aliases = {len(args): 0}
        args.append(dst)
    f = jnp.float32
    outs = [jax.ShapeDtypeStruct(p.shape, f)]
    row = jax.ShapeDtypeStruct((width, depth, lanes), f)
    slab = jax.ShapeDtypeStruct((rows, width, lanes), f)
    col = jax.ShapeDtypeStruct((rows, 1, depth, lanes), f)
    if final:
        outs += [jax.ShapeDtypeStruct((part, depth, lanes), f) for part in final]
    else:
        outs += [row, row, slab, slab] + [col, col] * around
    groups = width // GROUP
    cells = rows * width * depth * lanes

    def body(*refs):
        step_kernel(
            refs,
            start=start,
            width=width,
            total=total,
            final=final,
            has_dst=has_dst,
        )

    hbm = pl.BlockSpec(memory_space=pltpu.HBM)
    return pl.pallas_call(
        body,
        out_shape=outs,
        in_specs=[hbm] * len(args),
        out_specs=[hbm] * len(outs),
        scratch_shapes=[
            pltpu.VMEM((rows, width + (4 if around else 2), depth, lanes), f),
            pltpu.VMEM((rows, width, depth, lanes), f),
            pltpu.VMEM((rows, width, depth, lanes), f),
            pltpu.VMEM((3 if final else 2, width, depth, lanes), f),
            pltpu.VMEM((4, rows, width, lanes), f),
        ]
        + [pltpu.SemaphoreType.DMA((groups,))] * 4
        + [pltpu.SemaphoreType.DMA((2 + max(2, len(final)),)), pltpu.SemaphoreType.DMA((10,))],
        input_output_aliases=aliases,
        cost_estimate=pl.CostEstimate(
            flops=cells * 40, bytes_accessed=cells * 16, transcendentals=0
        ),
        name="wave_step",
    )(*args)


def sums_kernel(p_hbm, *refs, start, widths, total, count, has_dst):
    pieces = len(widths)
    before_hbm = refs[: count * pieces]
    refs = refs[count * pieces + (1 if has_dst else 0) :]
    out_hbm, pbuf, bbuf, psem, osem, bsem = refs
    rows = pbuf.shape[0]
    groups = sum(widths) // GROUP

    def there(g):
        return pl.ds(lax.rem(start + GROUP * g, total), GROUP)

    def field(g):
        return pltpu.make_async_copy(
            p_hbm.at[:, there(g)], pbuf.at[:, pl.ds(GROUP * g, GROUP)], psem.at[g]
        )

    def result(g):
        return pltpu.make_async_copy(
            pbuf.at[:, pl.ds(GROUP * g, GROUP)], out_hbm.at[:, there(g)], osem.at[g]
        )

    carried = []
    for a, width in enumerate(widths):
        for s in range(count):
            carried.append(
                pltpu.make_async_copy(
                    before_hbm[a * count + s],
                    bbuf.at[s, pl.ds(sum(widths[:a]), width)],
                    bsem.at[a * count + s],
                )
            )
    for cp in carried:
        cp.start()
    for g in range(groups):
        field(g).start()
    for cp in carried:
        cp.wait()

    def group(g, _):
        field(g).wait()

        def column(n, _):
            i = GROUP * g + n
            acc = bbuf[0, i]
            for s in range(1, count):
                acc = acc + bbuf[s, i]
            for j in range(rows):
                acc = acc + pbuf[j, i]
                pbuf[j, i] = acc * (1.0 / GRID_J)
            return 0

        lax.fori_loop(0, GROUP, column, 0)
        result(g).start()
        return 0

    lax.fori_loop(0, groups, group, 0)
    for g in range(groups):
        result(g).wait()


def sums(p, before, dst, *, start, widths):
    rows, total, depth, lanes = p.shape
    count = len(before[0])
    args = [p] + [b for piece in before for b in piece]
    aliases = {}
    if dst is not None:
        aliases = {len(args): 0}
        args.append(dst)
    width = sum(widths)
    groups = width // GROUP
    cells = rows * width * depth * lanes
    hbm = pl.BlockSpec(memory_space=pltpu.HBM)
    return pl.pallas_call(
        functools.partial(
            sums_kernel,
            start=start,
            widths=widths,
            total=total,
            count=count,
            has_dst=dst is not None,
        ),
        out_shape=jax.ShapeDtypeStruct(p.shape, jnp.float32),
        in_specs=[hbm] * len(args),
        out_specs=hbm,
        scratch_shapes=[
            pltpu.VMEM((rows, width, depth, lanes), jnp.float32),
            pltpu.VMEM((count, width, depth, lanes), jnp.float32),
        ]
        + [pltpu.SemaphoreType.DMA((groups,))] * 2
        + [pltpu.SemaphoreType.DMA((count * len(widths),))],
        input_output_aliases=aliases,
        cost_estimate=pl.CostEstimate(
            flops=cells * 10, bytes_accessed=cells * 8, transcendentals=0
        ),
        name="running_sums",
    )(*args)


def ring(axis, by):
    size = lax.axis_size(axis)
    return [(a, (a + by) % size) for a in range(size)]


def local(pressure, earlier, speed_square):
    rows, total, depth, _ = pressure.shape
    starts = [(total - WRAP + sum(WIDTHS[:a])) % total for a in range(len(WIDTHS))]
    chunks = list(zip(starts, WIDTHS))

    def exchange(edges, a):
        dn, up, kfirst, klast = edges[:4]
        got = [
            lax.ppermute(up, "rows", ring("rows", 1)),
            lax.ppermute(dn, "rows", ring("rows", -1)),
            lax.ppermute(klast, "slabs", ring("slabs", 1)),
            lax.ppermute(kfirst, "slabs", ring("slabs", -1)),
        ]
        if a == 0:
            ifirst, ilast = edges[4:]
            got += [
                lax.ppermute(ilast, "cols", ring("cols", 1)),
                lax.ppermute(ifirst, "cols", ring("cols", -1)),
            ]
        return got

    def start_edges(a):
        start, width = chunks[a]
        if a == 0:
            part = jnp.concatenate(
                [pressure[:, total - WRAP :], pressure[:, : width - WRAP]], axis=1
            )
        else:
            part = lax.slice_in_dim(pressure, start, start + width, axis=1)
        edges = [part[0], part[rows - 1], part[:, :, 0], part[:, :, depth - 1]]
        if a == 0:
            edges += [pressure[:, :1], pressure[:, total - 1 :]]
        return edges

    halos = [exchange(start_edges(a), a) for a in range(len(chunks))]
    older, newer = earlier, pressure
    for t in range(STEPS):
        final = t == STEPS - 1
        fresh = None if t < 2 else older
        made = []
        for a, (start, width) in enumerate(chunks):
            before = older if t < 2 else fresh
            fresh, *edges = step(
                newer,
                before,
                speed_square,
                halos[a],
                fresh,
                start=start,
                width=width,
                final=PIECES[a] if final else (),
            )
            made.append(edges if final else exchange(edges, a))
        older, newer = newer, fresh
        halos = made

    potential = None
    size = lax.axis_size("rows")
    for a, (start, width) in enumerate(chunks):
        carried_in = []
        for own in halos[a]:
            before, carried = [], own
            for s in range(size - 1):
                got = lax.ppermute(carried, "rows", [(s, s + 1)])
                before.append(got)
                carried = own + got
            carried_in.append(before)
        potential = sums(
            newer, carried_in, potential, start=start, widths=PIECES[a]
        )
    return potential, newer


def solution(mesh):
    placed = P(("site", "rows"), "cols", "slabs", None)

    return jax.shard_map(
        local,
        mesh=mesh,
        in_specs=(placed, placed, placed),
        out_specs=(placed, placed),
        check_vma=False,
    )
```

```python
import functools

import jax
import jax.numpy as jnp
from jax import lax
from jax.experimental import pallas as pl
from jax.experimental.pallas import tpu as pltpu
from jax.sharding import PartitionSpec as P


STEPS = 4
GRID_J = 16
WIDTHS = (32, 32)
WRAP = 16
GROUP = 8
PIECES = ((16, 16), (16, 8, 8))


def step_kernel(refs, *, start, width, total, place, final, has_dst):
    n = iter(range(len(refs)))

    def take():
        return refs[next(n)]

    around = start + width > total
    own = total - start if around else width
    p_hbm, e_hbm, c_hbm, lo_hbm, hi_hbm, klo_hbm, khi_hbm = (take() for _ in range(7))
    ilo_hbm, ihi_hbm = (take(), take()) if around else (None, None)
    if has_dst:
        take()
    if place and not final:
        take(), take()
    out_hbm = take()
    slab = (slice(None), pl.ds(place, width))
    if final:
        tot_hbm = [take() for _ in final]
    else:
        dn_hbm, up_hbm, kfirst_hbm, klast_hbm = (take() for _ in range(4))
        ifirst_hbm, ilast_hbm = (take(), take()) if around else (None, None)
    pbuf, ebuf, cbuf, rbuf, kbuf, psem, esem, csem, osem, rsem, ksem = (take() for _ in range(11))
    rows, depth = pbuf.shape[0], pbuf.shape[2]
    groups = width // GROUP

    def column_of(g):
        return lax.rem(start + GROUP * g, total)

    def shift_of(g):
        if not around:
            return 1
        if isinstance(g, int):
            return 1 if GROUP * g < own else 3
        return jnp.where(GROUP * g < own, 1, 3)

    def field(g, which):
        there = pl.ds(column_of(g), GROUP)
        src, buf, shift, sem = (
            (p_hbm, pbuf, shift_of(g), psem),
            (e_hbm, ebuf, 0, esem),
            (c_hbm, cbuf, 0, csem),
        )[which]
        return pltpu.make_async_copy(
            src.at[:, there], buf.at[:, pl.ds(GROUP * g + shift, GROUP)], sem.at[g]
        )

    def result(g):
        mine = pl.ds(GROUP * g, GROUP)
        return pltpu.make_async_copy(
            ebuf.at[:, mine], out_hbm.at[:, pl.ds(column_of(g), GROUP)], osem.at[g]
        )

    edge = pbuf.shape[1] - 1
    ends = [
        pltpu.make_async_copy(
            p_hbm.at[:, pl.ds(start - 1, 1)], pbuf.at[:, pl.ds(0, 1)], ksem.at[2]
        ),
        pltpu.make_async_copy(
            p_hbm.at[:, pl.ds((start + width) % total, 1)],
            pbuf.at[:, pl.ds(edge, 1)],
            ksem.at[3],
        ),
        pltpu.make_async_copy(klo_hbm.at[slab], kbuf.at[0], ksem.at[0]),
        pltpu.make_async_copy(khi_hbm.at[slab], kbuf.at[1], ksem.at[1]),
        pltpu.make_async_copy(lo_hbm, rbuf.at[0], rsem.at[0]),
        pltpu.make_async_copy(hi_hbm, rbuf.at[1], rsem.at[1]),
    ]
    if around:
        ends += [
            pltpu.make_async_copy(ihi_hbm, pbuf.at[:, pl.ds(own + 1, 1)], ksem.at[8]),
            pltpu.make_async_copy(ilo_hbm, pbuf.at[:, pl.ds(own + 2, 1)], ksem.at[9]),
        ]
    for which in range(3):
        field(0, which).start()
    for cp in ends:
        cp.start()
    for g in range(1, groups):
        for which in range(3):
            field(g, which).start()
    k = lax.broadcasted_iota(jnp.int32, (depth, pbuf.shape[3]), 0)
    is_first, is_last = k == 0, k == depth - 1
    for cp in ends:
        cp.wait()
    field(0, 0).wait()

    def group(g, _):
        @pl.when(g + 1 < groups)
        def _():
            field(g + 1, 0).wait()

        field(g, 1).wait()
        field(g, 2).wait()

        def column(n, _):
            i = GROUP * g + n
            at = i + shift_of(g)
            mid = [pbuf[j, at] for j in range(rows)]
            acc = None
            for j in range(rows):
                x = mid[j]
                low = rbuf[0, i] if j == 0 else mid[j - 1]
                high = rbuf[1, i] if j == rows - 1 else mid[j + 1]
                below = jnp.where(is_first, kbuf[0, j, pl.ds(i, 1), :], pltpu.roll(x, 1, 0))
                above = jnp.where(
                    is_last, kbuf[1, j, pl.ds(i, 1), :], pltpu.roll(x, depth - 1, 0)
                )
                spread = (
                    low + high + pbuf[j, at - 1] + pbuf[j, at + 1] + below + above - 6.0 * x
                )
                new = 2.0 * x - ebuf[j, i] + cbuf[j, i] * spread
                ebuf[j, i] = new
                if final:
                    acc = new if acc is None else acc + new
                else:
                    kbuf[2, j, pl.ds(i, 1), :] = new[0:1]
                    kbuf[3, j, pl.ds(i, 1), :] = new[depth - 1 : depth]
            if final:
                rbuf[2, i] = acc
            return 0

        lax.fori_loop(0, GROUP, column, 0)
        result(g).start()
        return 0

    lax.fori_loop(0, groups, group, 0)
    if final:
        edges = [
            pltpu.make_async_copy(
                rbuf.at[2, pl.ds(sum(final[:a]), final[a])], tot_hbm[a], rsem.at[2 + a]
            )
            for a in range(len(final))
        ]
    else:
        edges = [
            pltpu.make_async_copy(ebuf.at[0], dn_hbm, rsem.at[2]),
            pltpu.make_async_copy(ebuf.at[rows - 1], up_hbm, rsem.at[3]),
            pltpu.make_async_copy(kbuf.at[2], kfirst_hbm.at[slab], ksem.at[4]),
            pltpu.make_async_copy(kbuf.at[3], klast_hbm.at[slab], ksem.at[5]),
        ]
        if around:
            edges += [
                pltpu.make_async_copy(ebuf.at[:, pl.ds(own, 1)], ifirst_hbm, ksem.at[6]),
                pltpu.make_async_copy(ebuf.at[:, pl.ds(own - 1, 1)], ilast_hbm, ksem.at[7]),
            ]
    for cp in edges:
        cp.start()
    for g in range(groups):
        result(g).wait()
    for cp in edges:
        cp.wait()


def step(p, e, c, halo, dst, slabs, *, start, width, place, final):
    rows, total, depth, lanes = p.shape
    around = start + width > total
    args = [p, e, c, *halo]
    aliases = {}
    has_dst = dst is not None and dst is not e
    if dst is not None and not has_dst:
        aliases = {1: 0}
    elif has_dst:
        aliases = {len(args): 0}
        args.append(dst)
    if place and not final:
        aliases = {**aliases, len(args): 3, len(args) + 1: 4}
        args += slabs
    f = jnp.float32
    outs = [jax.ShapeDtypeStruct(p.shape, f)]
    row = jax.ShapeDtypeStruct((width, depth, lanes), f)
    slab = jax.ShapeDtypeStruct((rows, total, lanes), f)
    col = jax.ShapeDtypeStruct((rows, 1, depth, lanes), f)
    if final:
        outs += [jax.ShapeDtypeStruct((part, depth, lanes), f) for part in final]
    else:
        outs += [row, row, slab, slab] + [col, col] * around
    groups = width // GROUP
    cells = rows * width * depth * lanes

    def body(*refs):
        step_kernel(
            refs,
            start=start,
            width=width,
            total=total,
            place=place,
            final=final,
            has_dst=has_dst,
        )

    hbm = pl.BlockSpec(memory_space=pltpu.HBM)
    return pl.pallas_call(
        body,
        out_shape=outs,
        in_specs=[hbm] * len(args),
        out_specs=[hbm] * len(outs),
        scratch_shapes=[
            pltpu.VMEM((rows, width + (4 if around else 2), depth, lanes), f),
            pltpu.VMEM((rows, width, depth, lanes), f),
            pltpu.VMEM((rows, width, depth, lanes), f),
            pltpu.VMEM((3 if final else 2, width, depth, lanes), f),
            pltpu.VMEM((4, rows, width, lanes), f),
        ]
        + [pltpu.SemaphoreType.DMA((groups,))] * 4
        + [pltpu.SemaphoreType.DMA((2 + max(2, len(final)),)), pltpu.SemaphoreType.DMA((10,))],
        input_output_aliases=aliases,
        cost_estimate=pl.CostEstimate(
            flops=cells * 40, bytes_accessed=cells * 16, transcendentals=0
        ),
        name="wave_step",
    )(*args)


def sums_kernel(p_hbm, *refs, start, widths, total, count, has_dst):
    pieces = len(widths)
    before_hbm = refs[: count * pieces]
    refs = refs[count * pieces + (1 if has_dst else 0) :]
    out_hbm, pbuf, bbuf, psem, osem, bsem = refs
    rows = pbuf.shape[0]
    groups = sum(widths) // GROUP

    def there(g):
        return pl.ds(lax.rem(start + GROUP * g, total), GROUP)

    def field(g):
        return pltpu.make_async_copy(
            p_hbm.at[:, there(g)], pbuf.at[:, pl.ds(GROUP * g, GROUP)], psem.at[g]
        )

    def result(g):
        return pltpu.make_async_copy(
            pbuf.at[:, pl.ds(GROUP * g, GROUP)], out_hbm.at[:, there(g)], osem.at[g]
        )

    carried = []
    for a, width in enumerate(widths):
        for s in range(count):
            carried.append(
                pltpu.make_async_copy(
                    before_hbm[a * count + s],
                    bbuf.at[s, pl.ds(sum(widths[:a]), width)],
                    bsem.at[a * count + s],
                )
            )
    for cp in carried:
        cp.start()
    for g in range(groups):
        field(g).start()
    for cp in carried:
        cp.wait()

    def group(g, _):
        field(g).wait()

        def column(n, _):
            i = GROUP * g + n
            acc = bbuf[0, i]
            for s in range(1, count):
                acc = acc + bbuf[s, i]
            for j in range(rows):
                acc = acc + pbuf[j, i]
                pbuf[j, i] = acc * (1.0 / GRID_J)
            return 0

        lax.fori_loop(0, GROUP, column, 0)
        result(g).start()
        return 0

    lax.fori_loop(0, groups, group, 0)
    for g in range(groups):
        result(g).wait()


def sums(p, before, dst, *, start, widths):
    rows, total, depth, lanes = p.shape
    count = len(before[0])
    args = [p] + [b for piece in before for b in piece]
    aliases = {}
    if dst is not None:
        aliases = {len(args): 0}
        args.append(dst)
    width = sum(widths)
    groups = width // GROUP
    cells = rows * width * depth * lanes
    hbm = pl.BlockSpec(memory_space=pltpu.HBM)
    return pl.pallas_call(
        functools.partial(
            sums_kernel,
            start=start,
            widths=widths,
            total=total,
            count=count,
            has_dst=dst is not None,
        ),
        out_shape=jax.ShapeDtypeStruct(p.shape, jnp.float32),
        in_specs=[hbm] * len(args),
        out_specs=hbm,
        scratch_shapes=[
            pltpu.VMEM((rows, width, depth, lanes), jnp.float32),
            pltpu.VMEM((count, width, depth, lanes), jnp.float32),
        ]
        + [pltpu.SemaphoreType.DMA((groups,))] * 2
        + [pltpu.SemaphoreType.DMA((count * len(widths),))],
        input_output_aliases=aliases,
        cost_estimate=pl.CostEstimate(
            flops=cells * 10, bytes_accessed=cells * 8, transcendentals=0
        ),
        name="running_sums",
    )(*args)


def ring(axis, by):
    size = lax.axis_size(axis)
    return [(a, (a + by) % size) for a in range(size)]


def local(pressure, earlier, speed_square):
    rows, total, depth, _ = pressure.shape
    starts = [(total - WRAP + sum(WIDTHS[:a])) % total for a in range(len(WIDTHS))]
    chunks = list(zip(starts, WIDTHS))

    def exchange(edges, a):
        dn, up, kfirst, klast = edges[:4]
        got = [
            lax.ppermute(up, "rows", ring("rows", 1)), lax.ppermute(dn, "rows", ring("rows", -1))
        ]
        if a == 0:
            ifirst, ilast = edges[4:]
            got += [
                lax.ppermute(ilast, "cols", ring("cols", 1)),
                lax.ppermute(ifirst, "cols", ring("cols", -1)),
            ]
        if a == len(chunks) - 1:
            got += [
                lax.ppermute(klast, "slabs", ring("slabs", 1)),
                lax.ppermute(kfirst, "slabs", ring("slabs", -1)),
            ]
        return got

    def start_edges(a):
        start, width = chunks[a]

        def part(value, start, width, axis):
            if start + width <= total:
                return lax.slice_in_dim(value, start, start + width, axis=axis)
            own = total - start
            return jnp.concatenate(
                [
                    lax.slice_in_dim(value, start, total, axis=axis),
                    lax.slice_in_dim(value, 0, width - own, axis=axis),
                ],
                axis=axis,
            )

        edges = [part(pressure[j], start, width, 0) for j in (0, rows - 1)]
        edges += [part(pressure[:, :, k], starts[0], total, 1) for k in (0, depth - 1)]
        if a == 0:
            edges += [pressure[:, :1], pressure[:, total - 1 :]]
        return edges

    halos = [exchange(start_edges(a), a) for a in range(len(chunks))]
    older, newer = earlier, pressure
    for t in range(STEPS):
        final = t == STEPS - 1
        fresh = None if t < 2 else older
        made, slabs = [], []
        for a, (start, width) in enumerate(chunks):
            before = older if t < 2 else fresh
            halo = halos[a][:2] + halos[-1][-2:] + (halos[0][2:4] if a == 0 else [])
            fresh, *edges = step(
                newer,
                before,
                speed_square,
                halo,
                fresh,
                slabs,
                start=start,
                width=width,
                place=sum(WIDTHS[:a]),
                final=PIECES[a] if final else (),
            )
            slabs = edges[2:4]
            made.append(edges if final else exchange(edges, a))
        older, newer = newer, fresh
        halos = made

    potential = None
    size = lax.axis_size("rows")
    for a, (start, width) in enumerate(chunks):
        carried_in = []
        for own in halos[a]:
            before, carried = [], own
            for s in range(size - 1):
                got = lax.ppermute(carried, "rows", [(s, s + 1)])
                before.append(got)
                carried = own + got
            carried_in.append(before)
        potential = sums(
            newer, carried_in, potential, start=start, widths=PIECES[a]
        )
    return potential, newer


def solution(mesh):
    placed = P(("site", "rows"), "cols", "slabs", None)

    return jax.shard_map(
        local,
        mesh=mesh,
        in_specs=(placed, placed, placed),
        out_specs=(placed, placed),
        check_vma=False,
    )
```

```python
import functools

import jax
import jax.numpy as jnp
from jax import lax
from jax.experimental import pallas as pl
from jax.experimental.pallas import tpu as pltpu
from jax.sharding import PartitionSpec as P


STEPS = 4
GRID_J = 16
WIDTHS = (32, 32)
FIRST = 16
GROUP = 8
PIECES = ((16, 16), (16, 8, 8))


def step_kernel(refs, *, start, width, total, place, final, has_dst):
    n = iter(range(len(refs)))

    def take():
        return refs[next(n)]

    around = start + width > total
    own = total - start if around else width
    p_hbm, e_hbm, c_hbm, lo_hbm, hi_hbm, klo_hbm, khi_hbm = (take() for _ in range(7))
    ilo_hbm, ihi_hbm = (take(), take()) if around else (None, None)
    if has_dst:
        take()
    if place and not final:
        take(), take()
    out_hbm = take()
    slab = (slice(None), pl.ds(place, width))
    if final:
        tot_hbm = [take() for _ in final]
    else:
        dn_hbm, up_hbm, kfirst_hbm, klast_hbm = (take() for _ in range(4))
        ifirst_hbm, ilast_hbm = (take(), take()) if around else (None, None)
    pbuf, ebuf, cbuf, rbuf, kbuf, psem, esem, csem, osem, rsem, ksem = (take() for _ in range(11))
    rows, depth = pbuf.shape[0], pbuf.shape[2]
    groups = width // GROUP

    def column_of(g):
        return lax.rem(start + GROUP * g, total)

    def shift_of(g):
        if not around:
            return 1
        if isinstance(g, int):
            return 1 if GROUP * g < own else 3
        return jnp.where(GROUP * g < own, 1, 3)

    def field(g, which):
        there = pl.ds(column_of(g), GROUP)
        src, buf, shift, sem = (
            (p_hbm, pbuf, shift_of(g), psem),
            (e_hbm, ebuf, 0, esem),
            (c_hbm, cbuf, 0, csem),
        )[which]
        return pltpu.make_async_copy(
            src.at[:, there], buf.at[:, pl.ds(GROUP * g + shift, GROUP)], sem.at[g]
        )

    def result(g):
        mine = pl.ds(GROUP * g, GROUP)
        return pltpu.make_async_copy(
            ebuf.at[:, mine], out_hbm.at[:, pl.ds(column_of(g), GROUP)], osem.at[g]
        )

    edge = pbuf.shape[1] - 1
    ends = [
        pltpu.make_async_copy(
            p_hbm.at[:, pl.ds(start - 1, 1)], pbuf.at[:, pl.ds(0, 1)], ksem.at[2]
        ),
        pltpu.make_async_copy(
            p_hbm.at[:, pl.ds((start + width) % total, 1)],
            pbuf.at[:, pl.ds(edge, 1)],
            ksem.at[3],
        ),
        pltpu.make_async_copy(klo_hbm.at[slab], kbuf.at[0], ksem.at[0]),
        pltpu.make_async_copy(khi_hbm.at[slab], kbuf.at[1], ksem.at[1]),
        pltpu.make_async_copy(lo_hbm, rbuf.at[0], rsem.at[0]),
        pltpu.make_async_copy(hi_hbm, rbuf.at[1], rsem.at[1]),
    ]
    if around:
        ends += [
            pltpu.make_async_copy(ihi_hbm, pbuf.at[:, pl.ds(own + 1, 1)], ksem.at[8]),
            pltpu.make_async_copy(ilo_hbm, pbuf.at[:, pl.ds(own + 2, 1)], ksem.at[9]),
        ]
    for which in range(3):
        field(0, which).start()
    for cp in ends:
        cp.start()
    for g in range(1, groups):
        for which in range(3):
            field(g, which).start()
    k = lax.broadcasted_iota(jnp.int32, (depth, pbuf.shape[3]), 0)
    is_first, is_last = k == 0, k == depth - 1
    for cp in ends:
        cp.wait()
    field(0, 0).wait()

    def group(g, _):
        @pl.when(g + 1 < groups)
        def _():
            field(g + 1, 0).wait()

        field(g, 1).wait()
        field(g, 2).wait()

        def column(n, _):
            i = GROUP * g + n
            at = i + shift_of(g)
            mid = [pbuf[j, at] for j in range(rows)]
            acc = None
            for j in range(rows):
                x = mid[j]
                low = rbuf[0, i] if j == 0 else mid[j - 1]
                high = rbuf[1, i] if j == rows - 1 else mid[j + 1]
                below = jnp.where(is_first, kbuf[0, j, pl.ds(i, 1), :], pltpu.roll(x, 1, 0))
                above = jnp.where(
                    is_last, kbuf[1, j, pl.ds(i, 1), :], pltpu.roll(x, depth - 1, 0)
                )
                spread = (
                    low + high + pbuf[j, at - 1] + pbuf[j, at + 1] + below + above - 6.0 * x
                )
                new = 2.0 * x - ebuf[j, i] + cbuf[j, i] * spread
                ebuf[j, i] = new
                if final:
                    acc = new if acc is None else acc + new
                else:
                    kbuf[2, j, pl.ds(i, 1), :] = new[0:1]
                    kbuf[3, j, pl.ds(i, 1), :] = new[depth - 1 : depth]
            if final:
                rbuf[2, i] = acc
            return 0

        lax.fori_loop(0, GROUP, column, 0)
        result(g).start()
        return 0

    lax.fori_loop(0, groups, group, 0)
    if final:
        edges = [
            pltpu.make_async_copy(
                rbuf.at[2, pl.ds(sum(final[:a]), final[a])], tot_hbm[a], rsem.at[2 + a]
            )
            for a in range(len(final))
        ]
    else:
        edges = [
            pltpu.make_async_copy(ebuf.at[0], dn_hbm, rsem.at[2]),
            pltpu.make_async_copy(ebuf.at[rows - 1], up_hbm, rsem.at[3]),
            pltpu.make_async_copy(kbuf.at[2], kfirst_hbm.at[slab], ksem.at[4]),
            pltpu.make_async_copy(kbuf.at[3], klast_hbm.at[slab], ksem.at[5]),
        ]
        if around:
            edges += [
                pltpu.make_async_copy(ebuf.at[:, pl.ds(own, 1)], ifirst_hbm, ksem.at[6]),
                pltpu.make_async_copy(ebuf.at[:, pl.ds(own - 1, 1)], ilast_hbm, ksem.at[7]),
            ]
    for cp in edges:
        cp.start()
    for g in range(groups):
        result(g).wait()
    for cp in edges:
        cp.wait()


def step(p, e, c, halo, dst, slabs, *, start, width, place, final):
    rows, total, depth, lanes = p.shape
    around = start + width > total
    args = [p, e, c, *halo]
    aliases = {}
    has_dst = dst is not None and dst is not e
    if dst is not None and not has_dst:
        aliases = {1: 0}
    elif has_dst:
        aliases = {len(args): 0}
        args.append(dst)
    if place and not final:
        aliases = {**aliases, len(args): 3, len(args) + 1: 4}
        args += slabs
    f = jnp.float32
    outs = [jax.ShapeDtypeStruct(p.shape, f)]
    row = jax.ShapeDtypeStruct((width, depth, lanes), f)
    slab = jax.ShapeDtypeStruct((rows, total, lanes), f)
    col = jax.ShapeDtypeStruct((rows, 1, depth, lanes), f)
    if final:
        outs += [jax.ShapeDtypeStruct((part, depth, lanes), f) for part in final]
    else:
        outs += [row, row, slab, slab] + [col, col] * around
    groups = width // GROUP
    cells = rows * width * depth * lanes

    def body(*refs):
        step_kernel(
            refs,
            start=start,
            width=width,
            total=total,
            place=place,
            final=final,
            has_dst=has_dst,
        )

    hbm = pl.BlockSpec(memory_space=pltpu.HBM)
    return pl.pallas_call(
        body,
        out_shape=outs,
        in_specs=[hbm] * len(args),
        out_specs=[hbm] * len(outs),
        scratch_shapes=[
            pltpu.VMEM((rows, width + (4 if around else 2), depth, lanes), f),
            pltpu.VMEM((rows, width, depth, lanes), f),
            pltpu.VMEM((rows, width, depth, lanes), f),
            pltpu.VMEM((3 if final else 2, width, depth, lanes), f),
            pltpu.VMEM((4, rows, width, lanes), f),
        ]
        + [pltpu.SemaphoreType.DMA((groups,))] * 4
        + [pltpu.SemaphoreType.DMA((2 + max(2, len(final)),)), pltpu.SemaphoreType.DMA((10,))],
        input_output_aliases=aliases,
        cost_estimate=pl.CostEstimate(
            flops=cells * 40, bytes_accessed=cells * 16, transcendentals=0
        ),
        name="wave_step",
    )(*args)


def sums_kernel(p_hbm, *refs, start, widths, total, count, has_dst):
    pieces = len(widths)
    before_hbm = refs[: count * pieces]
    refs = refs[count * pieces + (1 if has_dst else 0) :]
    out_hbm, pbuf, bbuf, psem, osem, bsem = refs
    rows = pbuf.shape[0]
    groups = sum(widths) // GROUP

    def there(g):
        return pl.ds(lax.rem(start + GROUP * g, total), GROUP)

    def field(g):
        return pltpu.make_async_copy(
            p_hbm.at[:, there(g)], pbuf.at[:, pl.ds(GROUP * g, GROUP)], psem.at[g]
        )

    def result(g):
        return pltpu.make_async_copy(
            pbuf.at[:, pl.ds(GROUP * g, GROUP)], out_hbm.at[:, there(g)], osem.at[g]
        )

    carried = []
    for a, width in enumerate(widths):
        for s in range(count):
            carried.append(
                pltpu.make_async_copy(
                    before_hbm[a * count + s],
                    bbuf.at[s, pl.ds(sum(widths[:a]), width)],
                    bsem.at[a * count + s],
                )
            )
    for cp in carried:
        cp.start()
    for g in range(groups):
        field(g).start()
    for cp in carried:
        cp.wait()

    def group(g, _):
        field(g).wait()

        def column(n, _):
            i = GROUP * g + n
            acc = bbuf[0, i]
            for s in range(1, count):
                acc = acc + bbuf[s, i]
            for j in range(rows):
                acc = acc + pbuf[j, i]
                pbuf[j, i] = acc * (1.0 / GRID_J)
            return 0

        lax.fori_loop(0, GROUP, column, 0)
        result(g).start()
        return 0

    lax.fori_loop(0, groups, group, 0)
    for g in range(groups):
        result(g).wait()


def sums(p, before, dst, *, start, widths):
    rows, total, depth, lanes = p.shape
    count = len(before[0])
    args = [p] + [b for piece in before for b in piece]
    aliases = {}
    if dst is not None:
        aliases = {len(args): 0}
        args.append(dst)
    width = sum(widths)
    groups = width // GROUP
    cells = rows * width * depth * lanes
    hbm = pl.BlockSpec(memory_space=pltpu.HBM)
    return pl.pallas_call(
        functools.partial(
            sums_kernel,
            start=start,
            widths=widths,
            total=total,
            count=count,
            has_dst=dst is not None,
        ),
        out_shape=jax.ShapeDtypeStruct(p.shape, jnp.float32),
        in_specs=[hbm] * len(args),
        out_specs=hbm,
        scratch_shapes=[
            pltpu.VMEM((rows, width, depth, lanes), jnp.float32),
            pltpu.VMEM((count, width, depth, lanes), jnp.float32),
        ]
        + [pltpu.SemaphoreType.DMA((groups,))] * 2
        + [pltpu.SemaphoreType.DMA((count * len(widths),))],
        input_output_aliases=aliases,
        cost_estimate=pl.CostEstimate(
            flops=cells * 10, bytes_accessed=cells * 8, transcendentals=0
        ),
        name="running_sums",
    )(*args)


def ring(axis, by):
    size = lax.axis_size(axis)
    return [(a, (a + by) % size) for a in range(size)]


def local(pressure, earlier, speed_square):
    rows, total, depth, _ = pressure.shape
    starts = [FIRST + sum(WIDTHS[:a]) for a in range(len(WIDTHS))]
    chunks = list(zip(starts, WIDTHS))
    last = len(chunks) - 1

    def exchange(edges, a):
        dn, up, kfirst, klast = edges[:4]
        got = [
            lax.ppermute(up, "rows", ring("rows", 1)), lax.ppermute(dn, "rows", ring("rows", -1))
        ]
        if a == last:
            ifirst, ilast = edges[4:]
            got += [
                lax.ppermute(ilast, "cols", ring("cols", 1)),
                lax.ppermute(ifirst, "cols", ring("cols", -1)),
                lax.ppermute(klast, "slabs", ring("slabs", 1)),
                lax.ppermute(kfirst, "slabs", ring("slabs", -1)),
            ]
        return got

    def start_edges(a):
        start, width = chunks[a]

        def part(value, start, width, axis):
            if start + width <= total:
                return lax.slice_in_dim(value, start, start + width, axis=axis)
            own = total - start
            return jnp.concatenate(
                [
                    lax.slice_in_dim(value, start, total, axis=axis),
                    lax.slice_in_dim(value, 0, width - own, axis=axis),
                ],
                axis=axis,
            )

        edges = [part(pressure[j], start, width, 0) for j in (0, rows - 1)]
        edges += [part(pressure[:, :, k], starts[0], total, 1) for k in (0, depth - 1)]
        if a == last:
            edges += [pressure[:, :1], pressure[:, total - 1 :]]
        return edges

    halos = [exchange(start_edges(a), a) for a in range(len(chunks))]
    older, newer = earlier, pressure
    for t in range(STEPS):
        final = t == STEPS - 1
        fresh = None if t < 2 else older
        made, slabs = [], []
        for a, (start, width) in enumerate(chunks):
            before = older if t < 2 else fresh
            halo = halos[a][:2] + halos[last][4:] + (halos[last][2:4] if a == last else [])
            fresh, *edges = step(
                newer,
                before,
                speed_square,
                halo,
                fresh,
                slabs,
                start=start,
                width=width,
                place=sum(WIDTHS[:a]),
                final=PIECES[a] if final else (),
            )
            slabs = edges[2:4]
            made.append(edges if final else exchange(edges, a))
        older, newer = newer, fresh
        halos = made

    potential = None
    size = lax.axis_size("rows")
    for a, (start, width) in enumerate(chunks):
        carried_in = []
        for own in halos[a]:
            before, carried = [], own
            for s in range(size - 1):
                got = lax.ppermute(carried, "rows", [(s, s + 1)])
                before.append(got)
                carried = own + got
            carried_in.append(before)
        potential = sums(
            newer, carried_in, potential, start=start, widths=PIECES[a]
        )
    return potential, newer


def solution(mesh):
    placed = P(("site", "rows"), "cols", "slabs", None)

    return jax.shard_map(
        local,
        mesh=mesh,
        in_specs=(placed, placed, placed),
        out_specs=(placed, placed),
        check_vma=False,
    )
```

```python
import functools

import jax
import jax.numpy as jnp
from jax import lax
from jax.experimental import pallas as pl
from jax.experimental.pallas import tpu as pltpu
from jax.sharding import PartitionSpec as P


STEPS = 4
GRID_J = 16
WIDTHS = (32, 32)
FIRST = 16
GROUP = 8
VMEM_LIMIT = 16 * 2**20
PIECES = ((16, 16), (8, 8, 8, 8))


def step_kernel(refs, *, start, width, total, place, final, has_dst):
    n = iter(range(len(refs)))

    def take():
        return refs[next(n)]

    around = start + width > total
    own = total - start if around else width
    p_hbm, e_hbm, c_hbm, lo, hi, klo, khi = (take() for _ in range(7))
    ilo, ihi = (take(), take()) if around else (None, None)
    if has_dst:
        take()
    if place and not final:
        take(), take()
    out_hbm = take()
    slab = (slice(None), pl.ds(place, width))
    if final:
        tot_hbm = [take() for _ in final]
    else:
        dn_hbm, up_hbm, kfirst_hbm, klast_hbm = (take() for _ in range(4))
        ifirst_hbm, ilast_hbm = (take(), take()) if around else (None, None)
    pbuf, ebuf, cbuf, rbuf, kbuf, psem, esem, csem, osem, rsem, ksem = (take() for _ in range(11))
    rows, depth = pbuf.shape[0], pbuf.shape[2]
    groups = width // GROUP

    def column_of(g):
        return lax.rem(start + GROUP * g, total)

    def shift_of(g):
        if not around:
            return 1
        if isinstance(g, int):
            return 1 if GROUP * g < own else 3
        return jnp.where(GROUP * g < own, 1, 3)

    def field(g, which):
        there = pl.ds(column_of(g), GROUP)
        src, buf, shift, sem = (
            (p_hbm, pbuf, shift_of(g), psem),
            (e_hbm, ebuf, 0, esem),
            (c_hbm, cbuf, 0, csem),
        )[which]
        return pltpu.make_async_copy(
            src.at[:, there], buf.at[:, pl.ds(GROUP * g + shift, GROUP)], sem.at[g]
        )

    def result(g):
        mine = pl.ds(GROUP * g, GROUP)
        return pltpu.make_async_copy(
            ebuf.at[:, mine], out_hbm.at[:, pl.ds(column_of(g), GROUP)], osem.at[g]
        )

    edge = pbuf.shape[1] - 1
    ends = [
        pltpu.make_async_copy(
            p_hbm.at[:, pl.ds(start - 1, 1)], pbuf.at[:, pl.ds(0, 1)], ksem.at[2]
        ),
        pltpu.make_async_copy(
            p_hbm.at[:, pl.ds((start + width) % total, 1)],
            pbuf.at[:, pl.ds(edge, 1)],
            ksem.at[3],
        ),
    ]
    for which in range(3):
        field(0, which).start()
    for cp in ends:
        cp.start()
    for g in range(1, groups):
        for which in range(3):
            field(g, which).start()
    k = lax.broadcasted_iota(jnp.int32, (depth, pbuf.shape[3]), 0)
    is_first, is_last = k == 0, k == depth - 1
    if around:
        for j in range(rows):
            pbuf[j, own + 1] = ihi[j, 0]
            pbuf[j, own + 2] = ilo[j, 0]
    for cp in ends:
        cp.wait()
    field(0, 0).wait()

    def group(g, _):
        @pl.when(g + 1 < groups)
        def _():
            field(g + 1, 0).wait()

        field(g, 1).wait()
        field(g, 2).wait()

        def column(n, _):
            i = GROUP * g + n
            at = i + shift_of(g)
            mid = [pbuf[j, at] for j in range(rows)]
            acc = None
            for j in range(rows):
                x = mid[j]
                low = lo[i] if j == 0 else mid[j - 1]
                high = hi[i] if j == rows - 1 else mid[j + 1]
                below = jnp.where(is_first, klo[j, pl.ds(place + i, 1), :], pltpu.roll(x, 1, 0))
                above = jnp.where(
                    is_last, khi[j, pl.ds(place + i, 1), :], pltpu.roll(x, depth - 1, 0)
                )
                spread = (
                    low + high + pbuf[j, at - 1] + pbuf[j, at + 1] + below + above - 6.0 * x
                )
                new = 2.0 * x - ebuf[j, i] + cbuf[j, i] * spread
                ebuf[j, i] = new
                if final:
                    acc = new if acc is None else acc + new
                else:
                    kbuf[0, j, pl.ds(i, 1), :] = new[0:1]
                    kbuf[1, j, pl.ds(i, 1), :] = new[depth - 1 : depth]
            if final:
                rbuf[i] = acc
            return 0

        lax.fori_loop(0, GROUP, column, 0)
        result(g).start()
        return 0

    lax.fori_loop(0, groups, group, 0)
    if final:
        edges = [
            pltpu.make_async_copy(
                rbuf.at[pl.ds(sum(final[:a]), final[a])], tot_hbm[a], rsem.at[2 + a]
            )
            for a in range(len(final))
        ]
    else:
        edges = [
            pltpu.make_async_copy(ebuf.at[0], dn_hbm, rsem.at[2]),
            pltpu.make_async_copy(ebuf.at[rows - 1], up_hbm, rsem.at[3]),
            pltpu.make_async_copy(kbuf.at[0], kfirst_hbm.at[slab], ksem.at[4]),
            pltpu.make_async_copy(kbuf.at[1], klast_hbm.at[slab], ksem.at[5]),
        ]
        if around:
            edges += [
                pltpu.make_async_copy(ebuf.at[:, pl.ds(own, 1)], ifirst_hbm, ksem.at[6]),
                pltpu.make_async_copy(ebuf.at[:, pl.ds(own - 1, 1)], ilast_hbm, ksem.at[7]),
            ]
    for cp in edges:
        cp.start()
    for g in range(groups):
        result(g).wait()
    for cp in edges:
        cp.wait()


def step(p, e, c, halo, dst, slabs, *, start, width, place, final):
    rows, total, depth, lanes = p.shape
    around = start + width > total
    args = [p, e, c, *halo]
    aliases = {}
    has_dst = dst is not None and dst is not e
    if dst is not None and not has_dst:
        aliases = {1: 0}
    elif has_dst:
        aliases = {len(args): 0}
        args.append(dst)
    if place and not final:
        aliases = {**aliases, len(args): 3, len(args) + 1: 4}
        args += slabs
    f = jnp.float32
    outs = [jax.ShapeDtypeStruct(p.shape, f)]
    row = jax.ShapeDtypeStruct((width, depth, lanes), f)
    slab = jax.ShapeDtypeStruct((rows, total, lanes), f)
    col = jax.ShapeDtypeStruct((rows, 1, depth, lanes), f)
    if final:
        outs += [jax.ShapeDtypeStruct((part, depth, lanes), f) for part in final]
    else:
        outs += [row, row, slab, slab] + [col, col] * around
    groups = width // GROUP
    cells = rows * width * depth * lanes

    def body(*refs):
        step_kernel(
            refs,
            start=start,
            width=width,
            total=total,
            place=place,
            final=final,
            has_dst=has_dst,
        )

    hbm = pl.BlockSpec(memory_space=pltpu.HBM)
    return pl.pallas_call(
        body,
        out_shape=outs,
        in_specs=[hbm] * 3
        + [pl.BlockSpec(memory_space=pltpu.VMEM)] * len(halo)
        + [hbm] * (len(args) - 3 - len(halo)),
        out_specs=[hbm] * len(outs),
        compiler_params=pltpu.CompilerParams(vmem_limit_bytes=VMEM_LIMIT),
        scratch_shapes=[
            pltpu.VMEM((rows, width + (4 if around else 2), depth, lanes), f),
            pltpu.VMEM((rows, width, depth, lanes), f),
            pltpu.VMEM((rows, width, depth, lanes), f),
            pltpu.VMEM((width if final else 8, depth, lanes), f),
            pltpu.VMEM((2, rows, width, lanes), f),
        ]
        + [pltpu.SemaphoreType.DMA((groups,))] * 4
        + [pltpu.SemaphoreType.DMA((2 + max(2, len(final)),)), pltpu.SemaphoreType.DMA((10,))],
        input_output_aliases=aliases,
        cost_estimate=pl.CostEstimate(
            flops=cells * 40, bytes_accessed=cells * 16, transcendentals=0
        ),
        name="wave_step",
    )(*args)


def sums_kernel(p_hbm, *refs, start, widths, total, count, has_dst):
    pieces = len(widths)
    before = refs[: count * pieces]
    refs = refs[count * pieces + (1 if has_dst else 0) :]
    out_hbm, pbuf, psem, osem = refs
    rows = pbuf.shape[0]
    groups = sum(widths) // GROUP

    def there(g):
        return pl.ds(lax.rem(start + GROUP * g, total), GROUP)

    def field(g):
        return pltpu.make_async_copy(
            p_hbm.at[:, there(g)], pbuf.at[:, pl.ds(GROUP * g, GROUP)], psem.at[g]
        )

    def result(g):
        return pltpu.make_async_copy(
            pbuf.at[:, pl.ds(GROUP * g, GROUP)], out_hbm.at[:, there(g)], osem.at[g]
        )

    for g in range(groups):
        field(g).start()

    for a, width in enumerate(widths):
        first = sum(widths[:a])
        mine = before[a * count : (a + 1) * count]

        def group(g, _, first=first, mine=mine):
            field(g).wait()

            def column(n, _):
                i = GROUP * g + n
                acc = mine[0][i - first]
                for b in mine[1:]:
                    acc = acc + b[i - first]
                for j in range(rows):
                    acc = acc + pbuf[j, i]
                    pbuf[j, i] = acc * (1.0 / GRID_J)
                return 0

            lax.fori_loop(0, GROUP, column, 0)
            result(g).start()
            return 0

        lax.fori_loop(first // GROUP, (first + width) // GROUP, group, 0)
    for g in range(groups):
        result(g).wait()


def sums(p, before, dst, *, start, widths):
    rows, total, depth, lanes = p.shape
    count = len(before[0])
    args = [p] + [b for piece in before for b in piece]
    aliases = {}
    if dst is not None:
        aliases = {len(args): 0}
        args.append(dst)
    width = sum(widths)
    groups = width // GROUP
    cells = rows * width * depth * lanes
    hbm = pl.BlockSpec(memory_space=pltpu.HBM)
    return pl.pallas_call(
        functools.partial(
            sums_kernel,
            start=start,
            widths=widths,
            total=total,
            count=count,
            has_dst=dst is not None,
        ),
        out_shape=jax.ShapeDtypeStruct(p.shape, jnp.float32),
        in_specs=[hbm]
        + [pl.BlockSpec(memory_space=pltpu.VMEM)] * (count * len(widths))
        + [hbm] * len(aliases),
        out_specs=hbm,
        compiler_params=pltpu.CompilerParams(vmem_limit_bytes=VMEM_LIMIT),
        scratch_shapes=[pltpu.VMEM((rows, width, depth, lanes), jnp.float32)]
        + [pltpu.SemaphoreType.DMA((groups,))] * 2,
        input_output_aliases=aliases,
        cost_estimate=pl.CostEstimate(
            flops=cells * 10, bytes_accessed=cells * 8, transcendentals=0
        ),
        name="running_sums",
    )(*args)


def ring(axis, by):
    size = lax.axis_size(axis)
    return [(a, (a + by) % size) for a in range(size)]


def local(pressure, earlier, speed_square):
    rows, total, depth, _ = pressure.shape
    starts = [FIRST + sum(WIDTHS[:a]) for a in range(len(WIDTHS))]
    chunks = list(zip(starts, WIDTHS))
    last = len(chunks) - 1

    def exchange(edges, a):
        dn, up, kfirst, klast = edges[:4]
        got = [
            lax.ppermute(up, "rows", ring("rows", 1)), lax.ppermute(dn, "rows", ring("rows", -1))
        ]
        if a == last:
            ifirst, ilast = edges[4:]
            got += [
                lax.ppermute(ilast, "cols", ring("cols", 1)),
                lax.ppermute(ifirst, "cols", ring("cols", -1)),
                lax.ppermute(klast, "slabs", ring("slabs", 1)),
                lax.ppermute(kfirst, "slabs", ring("slabs", -1)),
            ]
        return got

    def start_edges(a):
        start, width = chunks[a]

        def part(value, start, width, axis):
            if start + width <= total:
                return lax.slice_in_dim(value, start, start + width, axis=axis)
            own = total - start
            return jnp.concatenate(
                [
                    lax.slice_in_dim(value, start, total, axis=axis),
                    lax.slice_in_dim(value, 0, width - own, axis=axis),
                ],
                axis=axis,
            )

        edges = [part(pressure[j], start, width, 0) for j in (0, rows - 1)]
        edges += [part(pressure[:, :, k], starts[0], total, 1) for k in (0, depth - 1)]
        if a == last:
            edges += [pressure[:, :1], pressure[:, total - 1 :]]
        return edges

    halos = [exchange(start_edges(a), a) for a in range(len(chunks))]
    older, newer = earlier, pressure
    for t in range(STEPS):
        final = t == STEPS - 1
        fresh = None if t < 2 else older
        made, slabs = [], []
        for a, (start, width) in enumerate(chunks):
            before = older if t < 2 else fresh
            halo = halos[a][:2] + halos[last][4:] + (halos[last][2:4] if a == last else [])
            fresh, *edges = step(
                newer,
                before,
                speed_square,
                halo,
                fresh,
                slabs,
                start=start,
                width=width,
                place=sum(WIDTHS[:a]),
                final=PIECES[a] if final else (),
            )
            slabs = edges[2:4]
            made.append(edges if final else exchange(edges, a))
        older, newer = newer, fresh
        halos = made

    potential = None
    size = lax.axis_size("rows")
    for a, (start, width) in enumerate(chunks):
        carried_in = []
        for own in halos[a]:
            before, carried = [], own
            for s in range(size - 1):
                got = lax.ppermute(carried, "rows", [(s, s + 1)])
                before.append(got)
                carried = own + got
            carried_in.append(before)
        potential = sums(
            newer, carried_in, potential, start=start, widths=PIECES[a]
        )
    return potential, newer


def solution(mesh):
    placed = P(("site", "rows"), "cols", "slabs", None)

    return jax.shard_map(
        local,
        mesh=mesh,
        in_specs=(placed, placed, placed),
        out_specs=(placed, placed),
        check_vma=False,
    )
```
